32 devices in a mesh: dp: 16 (over z, y, core), fsdp: 2 (over x).
Axes of the slice: x: 2, y: 2, z: 4, core: 2. Of those that a mesh axis runs over, the one named last changes fastest.
Arguments:
- patches: bfloat16 [16384, 768], P(('dp', 'fsdp')), may hold values from -6 to 6
- cotangent: bfloat16 [16384, 768], P(('dp', 'fsdp')), may hold values from -6 to 6
- lengths: int32 [32, 4], P(('dp', 'fsdp')), may hold values from 0 to 512, as said below
- arrange: int32 [16384], P(('dp', 'fsdp')), may hold values from 0 to 511, as said below
- first_gain: bfloat16 [768], P('dp'), may hold values from 0.3984375 to 1.59375
- first_shift: bfloat16 [768], P('dp'), may hold values from -1.5 to 1.5
- project_weight: bfloat16 [768, 2304], P('dp', 'fsdp'), may hold values from -0.21875 to 0.21875
- query_bias: bfloat16 [768], P('dp'), may hold values from -1.5 to 1.5
- value_bias: bfloat16 [768], P('dp'), may hold values from -1.5 to 1.5
- output_weight: bfloat16 [768, 768], P('dp', 'fsdp'), may hold values from -1.75 to 1.75
- output_bias: bfloat16 [768], P('dp'), may hold values from -1.5 to 1.5
- second_gain: bfloat16 [768], P('dp'), may hold values from 0.3984375 to 1.59375
- second_shift: bfloat16 [768], P('dp'), may hold values from -1.5 to 1.5
- up_weight: bfloat16 [768, 3072], P('dp', 'fsdp'), may hold values from -0.21875 to 0.21875
- up_bias: bfloat16 [3072], P('dp'), may hold values from -1.5 to 1.5
- down_weight: bfloat16 [3072, 768], P('dp', 'fsdp'), may hold values from -0.109375 to 0.109375
- down_bias: bfloat16 [768], P('dp'), may hold values from -1.5 to 1.5
Outputs:
- encoded: bfloat16 [16384, 768], P(('dp', 'fsdp'))
- grad_patches: bfloat16 [16384, 768], P(('dp', 'fsdp'))
- grad_first_gain: float32 [768], P('dp')
- grad_first_shift: float32 [768], P('dp')
- grad_project_weight: float32 [768, 2304], P('dp', 'fsdp')
- grad_query_bias: float32 [768], P('dp')
- grad_value_bias: float32 [768], P('dp')
- grad_output_weight: float32 [768, 768], P('dp', 'fsdp')
- grad_output_bias: float32 [768], P('dp')
- grad_second_gain: float32 [768], P('dp')
- grad_second_shift: float32 [768], P('dp')
- grad_up_weight: float32 [768, 3072], P('dp', 'fsdp')
- grad_up_bias: float32 [3072], P('dp')
- grad_down_weight: float32 [3072, 768], P('dp', 'fsdp')
- grad_down_bias: float32 [768], P('dp')
The draws below stay inside these ranges and needn't reach their ends.
Inputs may be any that keep to these rules, and one draw needn't show every extreme that they name: Each block's 4 lengths sum to at least 384 and at most 512; slots may be empty; in every draw some block holds a single sequence of 512 rows. `arrange`: each block's 512 entries are a permutation of 0 to 511.
All inputs are finite; a program needn't handle non-finite values.
Results may differ from the reference program's by a relative error of at most 0.012.
Values may be sent and summed in bfloat16 or wider, within the bound.
A program may use at most 128 MiB of HBM per device.

```python
import jax
import jax.numpy as jnp
from jax import lax

D = 768
HEADS = 12
HEAD = 64
FF = 3072
TOK_DEV = 512
SLOTS = 4
GROUPS = 32
PIECE = 32
ROWS = 16384
N_DP = 16
N_FSDP = 2


def draw_lengths(key, part):
    padding = jax.random.randint(jax.random.fold_in(key, 1), (GROUPS, 1), 0, TOK_DEV // 4 + 1)
    filled = TOK_DEV - padding
    cut_points = jax.random.randint(jax.random.fold_in(key, 2), (GROUPS, SLOTS - 1), 0, filled + 1)
    cut_points = jnp.sort(cut_points, axis=1)
    edges = jnp.concatenate([jnp.zeros((GROUPS, 1), jnp.int32), cut_points.astype(jnp.int32), filled.astype(jnp.int32)], axis=1)
    sizes_drawn = edges[:, 1:] - edges[:, :-1]
    full_block = jax.random.randint(jax.random.fold_in(key, 3), (), 0, GROUPS)
    single = jnp.zeros((SLOTS,), jnp.int32).at[0].set(TOK_DEV)
    chosen = (jnp.arange(GROUPS) == full_block)[:, None]
    return jnp.where(chosen, single[None, :], sizes_drawn).astype(jnp.int32)


def draw_arrange(key, part):
    block_keys = jax.random.split(jax.random.fold_in(key, 5), GROUPS)
    orders = jax.vmap(lambda one_key: jax.random.permutation(one_key, TOK_DEV))(block_keys)
    return orders.reshape(ROWS).astype(jnp.int32)


def levels(rng, shape, shards, low, largest):
    def one(axis_at, shards_of):
        draws = jax.random.uniform(jax.random.fold_in(jax.random.fold_in(rng, 6), axis_at), (shards_of,), jnp.float32, low / len(shards), largest / len(shards))
        return jnp.repeat(jnp.exp(draws), shape[axis_at] // shards_of).reshape((-1,) + (1,) * (len(shape) - axis_at - 1))

    factor_of = one(*shards[0])
    for cut in shards[1:]:
        factor_of = factor_of * one(*cut)
    return factor_of


def scatter_about(rng, dims, deviation, limit, pieces=(), held_as=jnp.bfloat16):
    array = deviation * jax.random.normal(rng, dims, jnp.float32)
    if pieces:
        array = array * levels(rng, dims, pieces, -0.22, 0.18)
    return jnp.clip(array, -limit, limit).astype(held_as)


def setup_inputs(seed: int = 0) -> dict:
    seeds = jax.random.split(jax.random.key(seed), 18)
    patches = scatter_about(seeds[0], (ROWS, D), 1.0, 6.0, ((0, 32),))
    cotangent = scatter_about(seeds[1], (ROWS, D), 1.0, 6.0, ((0, 32),))
    lengths = draw_lengths(jax.random.fold_in(seeds[17], 71), 0)
    arrange = draw_arrange(jax.random.fold_in(seeds[17], 71), 0)
    first_gain = jnp.clip(1.0 + 0.12 * jax.random.normal(seeds[4], (D,), jnp.float32), 0.3984375, 1.59375).astype(jnp.bfloat16)
    first_shift = scatter_about(seeds[5], (D,), 0.3, 1.5, ((0, 16),))
    project_weight = scatter_about(seeds[6], (D, 3 * D), D ** -0.5, 0.21875, ((0, 16), (1, 2)))
    query_bias = scatter_about(seeds[7], (D,), 0.3, 1.5, ((0, 16),))
    value_bias = scatter_about(seeds[8], (D,), 0.3, 1.5, ((0, 16),))
    output_weight = scatter_about(seeds[9], (D, D), (max(D // 64, 4)) ** -0.5, 1.75, ((0, 16), (1, 2)))
    output_bias = scatter_about(seeds[10], (D,), 0.3, 1.5, ((0, 16),))
    second_gain = jnp.clip(1.0 + 0.12 * jax.random.normal(seeds[11], (D,), jnp.float32), 0.3984375, 1.59375).astype(jnp.bfloat16)
    second_shift = scatter_about(seeds[12], (D,), 0.3, 1.5, ((0, 16),))
    up_weight = scatter_about(seeds[13], (D, FF), D ** -0.5, 0.21875, ((0, 16), (1, 2)))
    up_bias = scatter_about(seeds[14], (FF,), 0.3, 1.5, ((0, 16),))
    down_weight = scatter_about(seeds[15], (FF, D), FF ** -0.5, 0.109375, ((0, 16), (1, 2)))
    down_bias = scatter_about(seeds[16], (D,), 0.3, 1.5, ((0, 16),))
    return dict(patches=patches, cotangent=cotangent, lengths=lengths, arrange=arrange, first_gain=first_gain, first_shift=first_shift, project_weight=project_weight, query_bias=query_bias, value_bias=value_bias, output_weight=output_weight, output_bias=output_bias, second_gain=second_gain, second_shift=second_shift, up_weight=up_weight, up_bias=up_bias, down_weight=down_weight, down_bias=down_bias)


@jax.custom_vjp
def low(v):
    return lax.optimization_barrier(v.astype(jnp.bfloat16)).astype(jnp.float32)

@jax.custom_vjp
def low_back(v):
    return v

def low_keep(v):
    return (low(v), None)

def low_pass(kept, grad):
    return (grad,)

def back_keep(v):
    return (v, None)

def back_low(kept, grad):
    return (low(grad),)
low.defvjp(low_keep, low_pass)
low_back.defvjp(back_keep, back_low)
NORM_EPSILON = 1e-12
MASK_VALUE = -1e+30
ROOT_HALF = 0.7071067811865476

def high_dot(left_side, right_side):
    return jnp.dot(left_side, right_side, precision=lax.Precision.HIGHEST)

def norm_rows(values, norm_gain, norm_shift):
    center = values - lax.optimization_barrier(jnp.mean(values, axis=-1, keepdims=True))
    spread = lax.optimization_barrier(jnp.mean(center * center, axis=-1, keepdims=True))
    return center * lax.rsqrt(spread + NORM_EPSILON) * norm_gain + norm_shift

def gelu_exact(values):
    return 0.5 * values * (1.0 + lax.erf(values * ROOT_HALF))

def regroup(values):
    width = values.shape[-1]
    shaped = values.reshape(N_DP, N_FSDP, N_DP, PIECE, width)
    return jnp.transpose(shaped, (2, 1, 0, 3, 4)).reshape(ROWS, width)

def segment_labels(lengths, arrange):
    slot_ends = jnp.cumsum(lengths, axis=1)
    position = jnp.arange(TOK_DEV, dtype=jnp.int32)
    slot_index = lax.optimization_barrier(jnp.sum((position[None, :, None] >= slot_ends[:, None, :]).astype(jnp.int32), axis=2))
    orders = arrange.reshape(GROUPS, TOK_DEV)

    def place(order_row, slot_row):
        return jnp.zeros((TOK_DEV,), jnp.int32).at[order_row].set(slot_row)
    return jax.vmap(place)(orders, slot_index)

def encoder_layer(block_rows, labels, params):
    gain_one, shift_one, project_full, query_full, value_full, output_full, outbias_full, gain_two, shift_two, up_full, upbias_full, down_full, downbias_full = params
    width = block_rows.shape[1]
    live_rows = (labels < SLOTS).astype(jnp.float32)[:, None]
    normed_one = low(norm_rows(block_rows, gain_one, shift_one))
    joint = high_dot(normed_one, project_full)
    queries = low_back(low(joint[:, :width] + query_full))
    key_rows = low_back(low(joint[:, width:2 * width]))
    value_rows = low_back(low(joint[:, 2 * width:] + value_full))
    query_heads = queries.reshape(TOK_DEV, HEADS, HEAD)
    key_heads = key_rows.reshape(TOK_DEV, HEADS, HEAD)
    value_heads = value_rows.reshape(TOK_DEV, HEADS, HEAD)
    score_scale = HEAD ** (-0.5)
    raw_scores = jnp.einsum('qhe,khe->hqk', query_heads, key_heads, precision=lax.Precision.HIGHEST)
    scores = low_back(score_scale * raw_scores)
    visible = labels[:, None] == labels[None, :]
    masked = jnp.where(visible[None], scores, MASK_VALUE)
    top_score = lax.optimization_barrier(jnp.max(masked, axis=-1, keepdims=True))
    weights = jnp.exp(masked - top_score)
    prob_full = weights / lax.optimization_barrier(jnp.sum(weights, axis=-1, keepdims=True))
    prob_low = low(prob_full)
    mixed_rows = jnp.einsum('hqk,khe->qhe', prob_low, value_heads, precision=lax.Precision.HIGHEST)
    attended = low_back(low(mixed_rows.reshape(TOK_DEV, width)))
    attn_out = low_back(high_dot(attended, output_full) + outbias_full)
    hidden = block_rows + attn_out
    normed_two = low(norm_rows(hidden, gain_two, shift_two))
    pre_act = low_back(high_dot(normed_two, up_full) + upbias_full)
    activated = low(gelu_exact(pre_act))
    branch = low_back(high_dot(activated, down_full) + downbias_full)
    return live_rows * (hidden + branch)

def reference(patches, cotangent, lengths, arrange, first_gain, first_shift, project_weight, query_bias, value_bias, output_weight, output_bias, second_gain, second_shift, up_weight, up_bias, down_weight, down_bias):
    labels = segment_labels(lengths, arrange)
    inputs = regroup(patches.astype(jnp.float32))
    cot_rows = regroup(cotangent.astype(jnp.float32))
    params = tuple((item_value.astype(jnp.float32) for item_value in (first_gain, first_shift, project_weight, query_bias, value_bias, output_weight, output_bias, second_gain, second_shift, up_weight, up_bias, down_weight, down_bias)))

    def forward(rows_all, param_set):

        def one_block(block_pair):
            return encoder_layer(block_pair[0], block_pair[1], param_set)
        blocks = lax.map(jax.checkpoint(one_block), (rows_all.reshape(GROUPS, TOK_DEV, D), labels))
        return blocks.reshape(ROWS, D)
    out_rows, pull_back = jax.vjp(forward, inputs, params)
    grad_rows, grad_params = pull_back(cot_rows)
    encoded = regroup(out_rows).astype(jnp.bfloat16)
    grad_patches = regroup(grad_rows).astype(jnp.bfloat16)
    return (encoded, grad_patches, grad_params[0], grad_params[1], grad_params[2], grad_params[3], grad_params[4], grad_params[5], grad_params[6], grad_params[7], grad_params[8], grad_params[9], grad_params[10], grad_params[11], grad_params[12])
```

```python
import jax
import jax.numpy as jnp
from jax import lax
from jax.sharding import PartitionSpec as P

HEADS = 12
HEAD = 64


NORM_EPSILON = 1e-12
MASK_VALUE = -1e30
ROOT_HALF = 0.7071067811865476


def norm_rows(values, norm_gain, norm_shift):
    center = values - jnp.mean(values, axis=-1, keepdims=True)
    spread = jnp.mean(center * center, axis=-1, keepdims=True)
    return center * lax.rsqrt(spread + NORM_EPSILON) * norm_gain + norm_shift


def gelu_exact(values):
    return 0.5 * values * (1.0 + lax.erf(values * ROOT_HALF))


def slot_labels(lengths, arrange):
    total_rows = arrange.shape[0]
    slot_ends = jnp.cumsum(lengths[0])
    position = jnp.arange(total_rows, dtype=jnp.int32)
    slot_index = jnp.sum((position[:, None] >= slot_ends[None, :]).astype(jnp.int32), axis=1)
    return jnp.zeros((total_rows,), jnp.int32).at[arrange].set(slot_index)


def matmul(left_side, right_side, pattern):
    return jnp.einsum(pattern, left_side, right_side, preferred_element_type=jnp.float32)


def column_sums(values):
    return jnp.sum(values.astype(jnp.float32), axis=0)


def gather_matrix(block, n_dp, n_fsdp):
    rows, cols = block.shape
    every = lax.all_gather(block, ("dp", "fsdp"), axis=0, tiled=False)
    every = every.reshape(n_dp, n_fsdp, rows, cols).transpose(0, 2, 1, 3)
    return every.reshape(n_dp * rows, n_fsdp * cols)


def scatter_matrix(grad):
    part = lax.psum_scatter(grad.astype(jnp.bfloat16), "dp", scatter_dimension=0, tiled=True)
    part = lax.psum_scatter(part, "fsdp", scatter_dimension=1, tiled=True)
    return part.astype(jnp.float32)


def local(
    n_dp,
    n_fsdp,
    patches,
    cotangent,
    lengths,
    arrange,
    first_gain,
    first_shift,
    project_weight,
    query_bias,
    value_bias,
    output_weight,
    output_bias,
    second_gain,
    second_shift,
    up_weight,
    up_bias,
    down_weight,
    down_bias,
):
    arrived, cot_rows = (
        lax.all_to_all(patches, "dp", split_axis=0, concat_axis=0, tiled=True),
        lax.all_to_all(cotangent, "dp", split_axis=0, concat_axis=0, tiled=True),
    )
    total_rows, width = patches.shape
    labels = slot_labels(lengths, arrange)
    live_rows = (labels < lengths.shape[1]).astype(jnp.float32)[:, None]

    vector_parts = (
        first_gain, first_shift, query_bias, value_bias, output_bias,
        second_gain, second_shift, up_bias, down_bias,
    )
    widths = [v.shape[0] for v in vector_parts]
    packed = lax.all_gather(jnp.concatenate(vector_parts)[None], "dp", axis=0, tiled=True)
    vectors = []
    offset = 0
    for w in widths:
        vectors.append(packed[:, offset : offset + w].reshape(-1).astype(jnp.float32))
        offset += w
    gain_one, shift_one, query_full, value_full, outbias_full, gain_two, shift_two, upbias_full, downbias_full = vectors

    project_full = gather_matrix(project_weight, n_dp, n_fsdp)
    output_full = gather_matrix(output_weight, n_dp, n_fsdp)
    up_full = gather_matrix(up_weight, n_dp, n_fsdp)
    down_full = gather_matrix(down_weight, n_dp, n_fsdp)

    inputs = arrived.astype(jnp.float32)
    normed_one = norm_rows(inputs, gain_one, shift_one)
    normed_low = normed_one.astype(jnp.bfloat16)
    joint = jnp.dot(normed_low, project_full, preferred_element_type=jnp.float32)
    queries = (
        (joint[:, :width] + query_full).astype(jnp.bfloat16).reshape(total_rows, HEADS, HEAD)
    )
    key_rows = joint[:, width : 2 * width].astype(jnp.bfloat16).reshape(total_rows, HEADS, HEAD)
    value_rows = (
        (joint[:, 2 * width :] + value_full).astype(jnp.bfloat16).reshape(total_rows, HEADS, HEAD)
    )
    score_scale = HEAD ** (-0.5)
    visible = labels[:, None] == labels[None, :]

    def block_scores():
        raw_scores = matmul(queries, key_rows, "qhe,khe->hqk") * score_scale
        return jnp.where(visible[None], raw_scores, MASK_VALUE)

    scores = block_scores()
    top_score = jnp.max(scores, axis=-1, keepdims=True)
    weights = jnp.exp(scores - top_score)
    totals = jnp.sum(weights, axis=-1, keepdims=True)
    prob_low = (weights / totals).astype(jnp.bfloat16)
    mixed_rows = matmul(prob_low, value_rows, "hqk,khe->qhe")
    log_totals = top_score + jnp.log(totals)
    attended = mixed_rows.astype(jnp.bfloat16).reshape(total_rows, width)
    attn_out = jnp.dot(attended, output_full, preferred_element_type=jnp.float32) + outbias_full
    hidden = inputs + attn_out
    normed_two = norm_rows(hidden, gain_two, shift_two)
    normed_two_low = normed_two.astype(jnp.bfloat16)
    pre_act = jnp.dot(normed_two_low, up_full, preferred_element_type=jnp.float32) + upbias_full
    activated = gelu_exact(pre_act).astype(jnp.bfloat16)
    branch = jnp.dot(activated, down_full, preferred_element_type=jnp.float32) + downbias_full
    encoded_rows = live_rows * (hidden + branch)
    encoded_back = lax.all_to_all(
        encoded_rows.astype(jnp.bfloat16), "dp", split_axis=0, concat_axis=0, tiled=True
    )

    grad_out = live_rows * cot_rows.astype(jnp.float32)
    grad_branch = grad_out.astype(jnp.bfloat16)
    grad_down = matmul(activated, grad_branch, "tf,td->fd")
    grad_downbias = column_sums(grad_branch)
    grad_activ = matmul(grad_branch, down_full, "td,fd->tf")
    grad_pre = jax.vjp(gelu_exact, pre_act)[1](grad_activ)[0].astype(jnp.bfloat16)
    grad_up = matmul(normed_two_low, grad_pre, "td,tf->df")
    grad_upbias = column_sums(grad_pre)
    grad_normed_two = matmul(grad_pre, up_full, "tf,df->td")
    norm_pull_two = jax.vjp(norm_rows, hidden, gain_two, shift_two)[1]
    grad_hidden_part, grad_gain_two, grad_shift_two = norm_pull_two(grad_normed_two)
    grad_hidden = grad_out + grad_hidden_part
    down_low, up_low = grad_down.astype(jnp.bfloat16), grad_up.astype(jnp.bfloat16)
    grad_hidden, down_low, up_low = lax.optimization_barrier((grad_hidden, down_low, up_low))
    down_part = scatter_matrix(down_low)
    up_part = scatter_matrix(up_low)

    grad_attn = grad_hidden.astype(jnp.bfloat16)
    grad_output = matmul(attended, grad_attn, "td,te->de")
    grad_outbias = column_sums(grad_attn)
    grad_attended = (
        matmul(grad_attn, output_full, "te,de->td").astype(jnp.bfloat16).reshape(total_rows, HEADS, HEAD)
    )
    output_low = grad_output.astype(jnp.bfloat16)
    grad_attended, output_low = lax.optimization_barrier((grad_attended, output_low))
    output_part = scatter_matrix(output_low)

    scores = block_scores()
    prob_full = jnp.exp(scores - log_totals)
    prob_low = prob_full.astype(jnp.bfloat16)
    value_grad = matmul(prob_low, grad_attended, "hqk,qhe->khe")
    grad_prob = matmul(grad_attended, value_rows, "qhe,khe->hqk")
    inner = jnp.sum(prob_full * grad_prob, axis=-1, keepdims=True)
    grad_scores = (prob_full * (grad_prob - inner)).astype(jnp.bfloat16)
    query_grad = matmul(grad_scores, key_rows, "hqk,khe->qhe") * score_scale
    key_grad = matmul(grad_scores, queries, "hqk,qhe->khe") * score_scale
    grad_queries = query_grad.astype(jnp.bfloat16).reshape(total_rows, width)
    grad_keys = key_grad.reshape(total_rows, width).astype(jnp.bfloat16)
    grad_values = value_grad.reshape(total_rows, width).astype(jnp.bfloat16)
    grad_joint = jnp.concatenate([grad_queries, grad_keys, grad_values], axis=1)
    grad_project = matmul(normed_low, grad_joint, "td,tf->df")
    grad_querybias = column_sums(grad_queries)
    grad_valuebias = column_sums(grad_values)
    project_part = scatter_matrix(grad_project)
    grad_normed_one = matmul(grad_joint, project_full, "tf,df->td")
    norm_pull_one = jax.vjp(norm_rows, inputs, gain_one, shift_one)[1]
    grad_input_part, grad_gain_one, grad_shift_one = norm_pull_one(grad_normed_one)
    grad_inputs = grad_hidden + grad_input_part
    grad_back = lax.all_to_all(
        grad_inputs.astype(jnp.bfloat16), "dp", split_axis=0, concat_axis=0, tiled=True
    )

    vector_grads = (
        grad_gain_one, grad_shift_one, grad_querybias, grad_valuebias, grad_outbias,
        grad_gain_two, grad_shift_two, grad_upbias, grad_downbias,
    )
    stacked = jnp.concatenate([g.reshape(n_dp, -1) for g in vector_grads], axis=1)
    stacked = stacked + lax.ppermute(stacked, "fsdp", [(i, (i + 1) % n_fsdp) for i in range(n_fsdp)])
    mine = lax.psum_scatter(stacked, "dp", scatter_dimension=0, tiled=True)[0]
    sums = []
    offset = 0
    for w in widths:
        sums.append(mine[offset : offset + w])
        offset += w
    (g_gain_one, g_shift_one, g_querybias, g_valuebias, g_outbias,
     g_gain_two, g_shift_two, g_upbias, g_downbias) = sums

    return (
        encoded_back,
        grad_back,
        g_gain_one,
        g_shift_one,
        project_part,
        g_querybias,
        g_valuebias,
        output_part,
        g_outbias,
        g_gain_two,
        g_shift_two,
        up_part,
        g_upbias,
        down_part,
        g_downbias,
    )


def solution(mesh):
    n_dp, n_fsdp = mesh.shape["dp"], mesh.shape["fsdp"]
    rows = P(("dp", "fsdp"), None)
    matrix = P("dp", "fsdp")
    vector = P("dp")

    def step(*args):
        return local(n_dp, n_fsdp, *args)

    return jax.shard_map(
        step,
        mesh=mesh,
        in_specs=(rows, rows, rows, P(("dp", "fsdp")), vector, vector, matrix, vector, vector,
                  matrix, vector, vector, vector, matrix, vector, matrix, vector),
        out_specs=(rows, rows, vector, vector, matrix, vector, vector, matrix, vector, vector,
                   vector, matrix, vector, matrix, vector),
        check_vma=False,
    )
```

```python
import math

import jax
import jax.numpy as jnp
import numpy as np
from jax import lax
from jax.sharding import Mesh
from jax.sharding import PartitionSpec as P

HEADS = 12
HEAD = 64


NORM_EPSILON = 1e-12
MASK_VALUE = -1e30
ROOT_HALF = 0.7071067811865476


def norm_rows(values, norm_gain, norm_shift):
    center = values - jnp.mean(values, axis=-1, keepdims=True)
    spread = jnp.mean(center * center, axis=-1, keepdims=True)
    return center * lax.rsqrt(spread + NORM_EPSILON) * norm_gain + norm_shift


def gelu_exact(values):
    return 0.5 * values * (1.0 + lax.erf(values * ROOT_HALF))


def slot_labels(lengths, arrange):
    total_rows = arrange.shape[0]
    slot_ends = jnp.cumsum(lengths[0])
    position = jnp.arange(total_rows, dtype=jnp.int32)
    slot_index = jnp.sum((position[:, None] >= slot_ends[None, :]).astype(jnp.int32), axis=1)
    return jnp.zeros((total_rows,), jnp.int32).at[arrange].set(slot_index)


def matmul(left_side, right_side, pattern):
    return jnp.einsum(pattern, left_side, right_side, preferred_element_type=jnp.float32)


def column_sums(values):
    return jnp.sum(values.astype(jnp.float32), axis=0)


def physical_axes(mesh):
    line = mesh.devices[:, 0]
    n = len(line)

    def key(d):
        return (*d.coords, d.core_on_chip)

    try:
        first = key(line[0])
        found = []
        for ci in range(len(first)):
            values = {key(d)[ci] for d in line}
            if len(values) > 1:
                change = min(i for i in range(n) if key(line[i])[ci] != first[ci])
                found.append((change, len(values), ci))
        found.sort()
        stride = 1
        for change, size, _ in found:
            assert change == stride
            stride *= size
        assert stride == n
        sizes = [size for _, size, _ in found][::-1]
        core_at = [ci for _, _, ci in found][::-1].index(len(first) - 1)
    except (AssertionError, AttributeError, TypeError, ValueError):
        sizes, core_at = [n], None
    return sizes, core_at


class Tree:
    def __init__(self, canon, first, others, last):
        self.canon = canon
        self.first = first
        self.others = others
        self.last = last
        self.half = first[1] // 2 if first[1] % 2 == 0 else first[1]
        orders = [others, others[::-1]] if self.half < first[1] else [others]
        self.parts = []
        for order in orders:
            stages = list(order) + ([last] if last else [])
            self.parts.append(stages)

    def count(self):
        return math.prod(k for _, k in self.canon)

    def _part_axes(self, stages, size_first):
        return [ax for ax in stages[::-1]] + [(self.first[0], size_first)]

    def _index_tables(self):
        me = {name: lax.axis_index(name) for name, _ in self.canon}
        sizes = [k for _, k in self.canon]
        grids = jnp.meshgrid(*[jnp.arange(k, dtype=jnp.int32) for k in sizes], indexing="ij")
        actual = {name: g for (name, _), g in zip(self.canon, grids)}
        rel = {name: (me[name] - actual[name]) % k for name, k in self.canon}
        f_name = self.first[0]
        flat = jnp.zeros(sizes, jnp.int32)
        offset = 0
        pieces = []
        for p, stages in enumerate(self.parts):
            size_first = self.half if len(self.parts) > 1 else self.first[1]
            axes = self._part_axes(stages, size_first)
            index = jnp.zeros(sizes, jnp.int32)
            for name, k in axes:
                r = rel[name]
                if name == f_name:
                    r = r - p * self.half
                index = index * k + r
            pieces.append((offset, index))
            offset += math.prod(k for _, k in axes)
        if len(pieces) == 1:
            flat = pieces[0][1]
        else:
            in_first = rel[f_name] < self.half
            flat = jnp.where(in_first, pieces[0][1], pieces[1][0] + pieces[1][1])
        return flat.reshape(-1)

    def gather(self, block):
        f_name, f_k = self.first
        cur = _stage_gather(block, f_name, f_k)
        parts = []
        for p, stages in enumerate(self.parts):
            piece = cur[p * self.half : (p + 1) * self.half] if len(self.parts) > 1 else cur
            for name, k in stages:
                piece = _stage_gather(piece, name, k)
            parts.append(piece.reshape(-1, *block.shape))
        joined = jnp.concatenate(parts) if len(parts) > 1 else parts[0]
        return jnp.take(joined, self._index_tables(), axis=0)

    def scatter(self, blocks, send_dtype):
        table = self._index_tables()
        inverse = jnp.zeros_like(table).at[table].set(jnp.arange(table.shape[0], dtype=jnp.int32))
        relative = jnp.take(blocks, inverse, axis=0)
        shape = blocks.shape[1:]
        f_name, f_k = self.first
        ends = []
        offset = 0
        for p, stages in enumerate(self.parts):
            size_first = self.half if len(self.parts) > 1 else f_k
            axes = self._part_axes(stages, size_first)
            n = math.prod(k for _, k in axes)
            piece = relative[offset : offset + n].reshape(*[k for _, k in axes], *shape)
            offset += n
            for name, k in stages[::-1]:
                piece = _stage_scatter(piece, name, k, send_dtype)
            ends.append(piece)
        joined = jnp.concatenate(ends) if len(ends) > 1 else ends[0]
        return _stage_scatter(joined, f_name, f_k, send_dtype)


def _stage_gather(cur, name, k):
    outs = [cur] + [lax.ppermute(cur, name, [(i, (i + s) % k) for i in range(k)]) for s in range(1, k)]
    return jnp.stack(outs)


def _stage_scatter(cur, name, k, send_dtype):
    total = cur[0].astype(jnp.float32)
    for s in range(1, k):
        got = lax.ppermute(cur[s].astype(send_dtype), name, [(i, (i - s) % k) for i in range(k)])
        total = total + got.astype(jnp.float32)
    return total


def build(mesh):
    n_dp, n_fsdp = mesh.shape["dp"], mesh.shape["fsdp"]
    sizes, core_at = physical_axes(mesh)
    names = [f"d{i}" for i in range(len(sizes))]
    phys = Mesh(mesh.devices.reshape(*sizes, n_fsdp), (*names, "fsdp"))
    dp_axes = list(zip(names, sizes))
    last = dp_axes[core_at] if core_at is not None and len(dp_axes) > 1 else None
    external = [ax for ax in dp_axes if ax != last]
    first = max(external, key=lambda ax: ax[1])
    rest = [ax for ax in external if ax != first]
    weights = Tree([("fsdp", n_fsdp)] + dp_axes, first, rest + [("fsdp", n_fsdp)], last)
    vectors = Tree(dp_axes, first, rest, last)
    return phys, tuple(names), weights, vectors


def local(dp_names, weights_tree, vectors_tree, n_dp, n_fsdp, patches, cotangent, lengths, arrange,
          first_gain, first_shift, project_weight, query_bias, value_bias, output_weight, output_bias,
          second_gain, second_shift, up_weight, up_bias, down_weight, down_bias):
    arrived = lax.all_to_all(patches, dp_names, split_axis=0, concat_axis=0, tiled=True)
    cot_rows = lax.all_to_all(cotangent, dp_names, split_axis=0, concat_axis=0, tiled=True)
    total_rows, width = patches.shape
    labels = slot_labels(lengths, arrange)
    live_rows = (labels < lengths.shape[1]).astype(jnp.float32)[:, None]

    vector_parts = (
        first_gain, first_shift, query_bias, value_bias, output_bias,
        second_gain, second_shift, up_bias, down_bias,
    )
    widths = [v.shape[0] for v in vector_parts]
    packed = vectors_tree.gather(jnp.concatenate(vector_parts))
    vectors = []
    offset = 0
    for w in widths:
        vectors.append(packed[:, offset : offset + w].reshape(-1).astype(jnp.float32))
        offset += w
    gain_one, shift_one, query_full, value_full, outbias_full, gain_two, shift_two, upbias_full, downbias_full = vectors

    def gather_matrix(block):
        rows, cols = block.shape
        every = weights_tree.gather(block)
        return every.reshape(n_fsdp, n_dp * rows, cols)

    project_full = gather_matrix(project_weight)
    output_full = gather_matrix(output_weight)
    up_full = gather_matrix(up_weight)
    down_full = gather_matrix(down_weight)

    def split_cols(values):
        return values.reshape(values.shape[0], n_fsdp, -1)

    def forward_dot(left, matrix):
        out = matmul(left, matrix, "td,jdc->tjc")
        return out.reshape(out.shape[0], -1)

    def backward_dot(grad, matrix):
        return matmul(split_cols(grad), matrix, "tjc,jdc->td")

    def weight_grad(left, grad):
        out = matmul(left, split_cols(grad), "td,tjc->jdc")
        return out.astype(jnp.bfloat16)

    def scatter_matrix(grad_low, rows):
        blocks = grad_low.reshape(n_fsdp * n_dp, rows, grad_low.shape[-1])
        return weights_tree.scatter(blocks, jnp.bfloat16)

    inputs = arrived.astype(jnp.float32)
    normed_one = norm_rows(inputs, gain_one, shift_one)
    normed_low = normed_one.astype(jnp.bfloat16)
    joint = forward_dot(normed_low, project_full)
    queries = (joint[:, :width] + query_full).astype(jnp.bfloat16).reshape(total_rows, HEADS, HEAD)
    key_rows = joint[:, width : 2 * width].astype(jnp.bfloat16).reshape(total_rows, HEADS, HEAD)
    value_rows = (joint[:, 2 * width :] + value_full).astype(jnp.bfloat16).reshape(total_rows, HEADS, HEAD)
    score_scale = HEAD ** (-0.5)
    visible = labels[:, None] == labels[None, :]

    def block_scores():
        raw_scores = matmul(queries, key_rows, "qhe,khe->hqk") * score_scale
        return jnp.where(visible[None], raw_scores, MASK_VALUE)

    scores = block_scores()
    top_score = jnp.max(scores, axis=-1, keepdims=True)
    weights = jnp.exp(scores - top_score)
    totals = jnp.sum(weights, axis=-1, keepdims=True)
    prob_low = (weights / totals).astype(jnp.bfloat16)
    mixed_rows = matmul(prob_low, value_rows, "hqk,khe->qhe")
    log_totals = top_score + jnp.log(totals)
    attended = mixed_rows.astype(jnp.bfloat16).reshape(total_rows, width)
    attn_out = forward_dot(attended, output_full) + outbias_full
    hidden = inputs + attn_out
    normed_two = norm_rows(hidden, gain_two, shift_two)
    normed_two_low = normed_two.astype(jnp.bfloat16)
    pre_act = forward_dot(normed_two_low, up_full) + upbias_full
    activated = gelu_exact(pre_act).astype(jnp.bfloat16)
    branch = forward_dot(activated, down_full) + downbias_full
    encoded_rows = live_rows * (hidden + branch)
    encoded_back = lax.all_to_all(
        encoded_rows.astype(jnp.bfloat16), dp_names, split_axis=0, concat_axis=0, tiled=True
    )

    grad_out = live_rows * cot_rows.astype(jnp.float32)
    grad_branch = grad_out.astype(jnp.bfloat16)
    down_low = weight_grad(activated, grad_branch)
    grad_downbias = column_sums(grad_branch)
    grad_activ = backward_dot(grad_branch, down_full)
    grad_pre = jax.vjp(gelu_exact, pre_act)[1](grad_activ)[0].astype(jnp.bfloat16)
    up_low = weight_grad(normed_two_low, grad_pre)
    grad_upbias = column_sums(grad_pre)
    grad_normed_two = backward_dot(grad_pre, up_full)
    norm_pull_two = jax.vjp(norm_rows, hidden, gain_two, shift_two)[1]
    grad_hidden_part, grad_gain_two, grad_shift_two = norm_pull_two(grad_normed_two)
    grad_hidden = grad_out + grad_hidden_part
    grad_hidden, down_low, up_low = lax.optimization_barrier((grad_hidden, down_low, up_low))
    down_part = scatter_matrix(down_low, down_weight.shape[0])
    up_part = scatter_matrix(up_low, up_weight.shape[0])

    grad_attn = grad_hidden.astype(jnp.bfloat16)
    output_low = weight_grad(attended, grad_attn)
    grad_outbias = column_sums(grad_attn)
    grad_attended = backward_dot(grad_attn, output_full).astype(jnp.bfloat16).reshape(total_rows, HEADS, HEAD)
    grad_attended, output_low = lax.optimization_barrier((grad_attended, output_low))
    output_part = scatter_matrix(output_low, output_weight.shape[0])

    scores = block_scores()
    prob_full = jnp.exp(scores - log_totals)
    prob_low = prob_full.astype(jnp.bfloat16)
    value_grad = matmul(prob_low, grad_attended, "hqk,qhe->khe")
    grad_prob = matmul(grad_attended, value_rows, "qhe,khe->hqk")
    inner = jnp.sum(prob_full * grad_prob, axis=-1, keepdims=True)
    grad_scores = (prob_full * (grad_prob - inner)).astype(jnp.bfloat16)
    query_grad = matmul(grad_scores, key_rows, "hqk,khe->qhe") * score_scale
    key_grad = matmul(grad_scores, queries, "hqk,qhe->khe") * score_scale
    grad_queries = query_grad.astype(jnp.bfloat16).reshape(total_rows, width)
    grad_keys = key_grad.reshape(total_rows, width).astype(jnp.bfloat16)
    grad_values = value_grad.reshape(total_rows, width).astype(jnp.bfloat16)
    grad_joint = jnp.concatenate([grad_queries, grad_keys, grad_values], axis=1)
    project_low = weight_grad(normed_low, grad_joint)
    grad_querybias = column_sums(grad_queries)
    grad_valuebias = column_sums(grad_values)
    project_part = scatter_matrix(project_low, project_weight.shape[0])
    grad_normed_one = backward_dot(grad_joint, project_full)
    norm_pull_one = jax.vjp(norm_rows, inputs, gain_one, shift_one)[1]
    grad_input_part, grad_gain_one, grad_shift_one = norm_pull_one(grad_normed_one)
    grad_inputs = grad_hidden + grad_input_part
    grad_back = lax.all_to_all(
        grad_inputs.astype(jnp.bfloat16), dp_names, split_axis=0, concat_axis=0, tiled=True
    )

    vector_grads = (
        grad_gain_one, grad_shift_one, grad_querybias, grad_valuebias, grad_outbias,
        grad_gain_two, grad_shift_two, grad_upbias, grad_downbias,
    )
    stacked = jnp.concatenate([g.reshape(n_dp, -1) for g in vector_grads], axis=1)
    stacked = stacked + lax.ppermute(stacked, "fsdp", [(i, (i + 1) % n_fsdp) for i in range(n_fsdp)])
    mine = vectors_tree.scatter(stacked, jnp.float32)
    sums = []
    offset = 0
    for w in widths:
        sums.append(mine[offset : offset + w])
        offset += w
    (g_gain_one, g_shift_one, g_querybias, g_valuebias, g_outbias,
     g_gain_two, g_shift_two, g_upbias, g_downbias) = sums

    return (
        encoded_back, grad_back, g_gain_one, g_shift_one, project_part, g_querybias, g_valuebias,
        output_part, g_outbias, g_gain_two, g_shift_two, up_part, g_upbias, down_part, g_downbias,
    )


def solution(mesh):
    n_dp, n_fsdp = mesh.shape["dp"], mesh.shape["fsdp"]
    phys, dp_names, weights_tree, vectors_tree = build(mesh)
    rows = P((*dp_names, "fsdp"), None)
    matrix = P(dp_names, "fsdp")
    vector = P(dp_names)

    def step(*args):
        return local(dp_names, weights_tree, vectors_tree, n_dp, n_fsdp, *args)

    return jax.shard_map(
        step,
        mesh=phys,
        in_specs=(rows, rows, rows, P((*dp_names, "fsdp")), vector, vector, matrix, vector, vector,
                  matrix, vector, vector, vector, matrix, vector, matrix, vector),
        out_specs=(rows, rows, vector, vector, matrix, vector, vector, matrix, vector, vector,
                   vector, matrix, vector, matrix, vector),
        check_vma=False,
    )
```

```python
import math

import jax
import jax.numpy as jnp
import numpy as np
from jax import lax
from jax.sharding import Mesh
from jax.sharding import PartitionSpec as P

HEADS = 12
HEAD = 64


NORM_EPSILON = 1e-12
MASK_VALUE = -1e30
ROOT_HALF = 0.7071067811865476


def norm_rows(values, norm_gain, norm_shift):
    center = values - jnp.mean(values, axis=-1, keepdims=True)
    spread = jnp.mean(center * center, axis=-1, keepdims=True)
    return center * lax.rsqrt(spread + NORM_EPSILON) * norm_gain + norm_shift


def gelu_exact(values):
    return 0.5 * values * (1.0 + lax.erf(values * ROOT_HALF))


def slot_labels(lengths, arrange):
    total_rows = arrange.shape[0]
    slot_ends = jnp.cumsum(lengths[0])
    position = jnp.arange(total_rows, dtype=jnp.int32)
    slot_index = jnp.sum((position[:, None] >= slot_ends[None, :]).astype(jnp.int32), axis=1)
    return jnp.zeros((total_rows,), jnp.int32).at[arrange].set(slot_index)


def matmul(left_side, right_side, pattern):
    return jnp.einsum(pattern, left_side, right_side, preferred_element_type=jnp.float32)


def column_sums(values):
    return jnp.sum(values.astype(jnp.float32), axis=0)


def physical_axes(mesh):
    line = mesh.devices[:, 0]
    n = len(line)

    def key(d):
        return (*d.coords, d.core_on_chip)

    try:
        first = key(line[0])
        found = []
        for ci in range(len(first)):
            values = {key(d)[ci] for d in line}
            if len(values) > 1:
                change = min(i for i in range(n) if key(line[i])[ci] != first[ci])
                found.append((change, len(values), ci))
        found.sort()
        stride = 1
        for change, size, _ in found:
            assert change == stride
            stride *= size
        assert stride == n
        sizes = [size for _, size, _ in found][::-1]
        core_at = [ci for _, _, ci in found][::-1].index(len(first) - 1)
    except (AssertionError, AttributeError, TypeError, ValueError):
        sizes, core_at = [n], None
    return sizes, core_at


class Tree:
    def __init__(self, canon, first, others, last):
        self.canon = canon
        self.pos = {name: i for i, (name, _) in enumerate(canon)}
        self.size = dict(canon)
        self.sizes = [k for _, k in canon]
        self.first = first
        self.last = last
        split = first[1] % 2 == 0 and len(others) > 1
        self.half = first[1] // 2 if split else first[1]
        orders = [others, others[::-1]] if split else [others]
        self.parts = [list(order) + ([last] if last else []) for order in orders]

    def _me(self, name):
        return lax.axis_index(name)

    def _insert(self, present, name):
        new = sorted(present + [name], key=lambda n: self.pos[n])
        return new.index(name), new

    def _gather_stage(self, cur, present, name):
        k = self.size[name]
        at, present = self._insert(present, name)
        outs = [cur] + [lax.ppermute(cur, name, [(i, (i + s) % k) for i in range(k)]) for s in range(1, k)]
        me = self._me(name)
        if k == 2:
            new = jnp.where(me == 0, jnp.stack(outs, axis=at), jnp.stack(outs[::-1], axis=at))
        else:
            order = (me - jnp.arange(k, dtype=jnp.int32)) % k
            new = jnp.take(jnp.stack(outs, axis=at), order, axis=at, mode="clip")
        return new, present

    def gather(self, block):
        f_name, f_k = self.first
        cur, present = self._gather_stage(block, [], f_name)
        at = present.index(f_name)
        pieces = []
        for p, stages in enumerate(self.parts):
            piece = lax.slice_in_dim(cur, p * self.half, (p + 1) * self.half, axis=at) if len(self.parts) > 1 else cur
            got = [f_name]
            for name in [n for n, _ in stages]:
                piece, got = self._gather_stage(piece, got, name)
            pieces.append(piece)
        if len(pieces) == 1:
            return pieces[0]
        return jnp.concatenate(pieces, axis=self.pos[f_name])

    def _scatter_stage(self, cur, present, name, send_dtype):
        k = self.size[name]
        at = present.index(name)
        me = self._me(name)
        total = lax.dynamic_index_in_dim(cur, me, axis=at, keepdims=False).astype(jnp.float32)
        for s in range(1, k):
            slab = lax.dynamic_index_in_dim(cur, (me + s) % k, axis=at, keepdims=False)
            got = lax.ppermute(slab.astype(send_dtype), name, [(i, (i + s) % k) for i in range(k)])
            total = total + got.astype(jnp.float32)
        return total, [n for n in present if n != name]

    def scatter(self, blocks, send_dtype):
        present = [n for n, _ in self.canon]
        f_name = self.first[0]
        cur = blocks
        if self.last:
            cur, present = self._scatter_stage(cur, present, self.last[0], send_dtype)
        at = present.index(f_name)
        ends = []
        for p, stages in enumerate(self.parts):
            piece = lax.slice_in_dim(cur, p * self.half, (p + 1) * self.half, axis=at) if len(self.parts) > 1 else cur
            have = list(present)
            for name in [n for n, _ in stages if n != (self.last[0] if self.last else None)][::-1]:
                piece, have = self._scatter_stage(piece, have, name, send_dtype)
            ends.append(piece)
        joined = jnp.concatenate(ends, axis=0) if len(ends) > 1 else ends[0]
        total, _ = self._scatter_stage(joined, [f_name], f_name, send_dtype)
        return total


def build(mesh):
    n_dp, n_fsdp = mesh.shape["dp"], mesh.shape["fsdp"]
    sizes, core_at = physical_axes(mesh)
    names = [f"d{i}" for i in range(len(sizes))]
    phys = Mesh(mesh.devices.reshape(*sizes, n_fsdp), (*names, "fsdp"))
    dp_axes = list(zip(names, sizes))
    last = dp_axes[core_at] if core_at is not None and len(dp_axes) > 1 else None
    external = [ax for ax in dp_axes if ax != last]
    first = max(external, key=lambda ax: ax[1])
    rest = [ax for ax in external if ax != first]
    weights = Tree([("fsdp", n_fsdp)] + dp_axes, first, rest + [("fsdp", n_fsdp)], last)
    vectors = Tree(dp_axes, first, rest, last)
    return phys, tuple(names), weights, vectors


def local(dp_names, weights_tree, vectors_tree, n_dp, n_fsdp, patches, cotangent, lengths, arrange,
          first_gain, first_shift, project_weight, query_bias, value_bias, output_weight, output_bias,
          second_gain, second_shift, up_weight, up_bias, down_weight, down_bias):
    arrived = lax.all_to_all(patches, dp_names, split_axis=0, concat_axis=0, tiled=True)
    cot_rows = lax.all_to_all(cotangent, dp_names, split_axis=0, concat_axis=0, tiled=True)
    total_rows, width = patches.shape
    labels = slot_labels(lengths, arrange)
    live_rows = (labels < lengths.shape[1]).astype(jnp.float32)[:, None]

    vector_parts = (
        first_gain, first_shift, query_bias, value_bias, output_bias,
        second_gain, second_shift, up_bias, down_bias,
    )
    widths = [v.shape[0] for v in vector_parts]
    packed = vectors_tree.gather(jnp.concatenate(vector_parts)).reshape(n_dp, -1)
    vectors = []
    offset = 0
    for w in widths:
        vectors.append(packed[:, offset : offset + w].reshape(-1).astype(jnp.float32))
        offset += w
    gain_one, shift_one, query_full, value_full, outbias_full, gain_two, shift_two, upbias_full, downbias_full = vectors

    def gather_matrix(block):
        rows, cols = block.shape
        every = weights_tree.gather(block)
        return every.reshape(n_fsdp, n_dp * rows, cols)

    project_full = gather_matrix(project_weight)
    output_rows = output_weight.shape[0]
    both = weights_tree.gather(jnp.concatenate([output_weight, down_weight], axis=0))
    output_full = both[..., :output_rows, :].reshape(n_fsdp, n_dp * output_rows, -1)
    down_full = both[..., output_rows:, :].reshape(n_fsdp, -1, down_weight.shape[1])
    up_full = gather_matrix(up_weight)

    def split_cols(values):
        return values.reshape(values.shape[0], n_fsdp, -1)

    def forward_dot(left, matrix):
        out = matmul(left, matrix, "td,jdc->tjc")
        return out.reshape(out.shape[0], -1)

    def backward_dot(grad, matrix):
        return matmul(split_cols(grad), matrix, "tjc,jdc->td")

    def weight_grad(left, grad):
        out = matmul(left, split_cols(grad), "td,tjc->jdc")
        return out.astype(jnp.bfloat16)

    def scatter_matrix(grad_low, rows):
        blocks = grad_low.reshape(*weights_tree.sizes, rows, grad_low.shape[-1])
        return weights_tree.scatter(blocks, jnp.bfloat16)

    inputs = arrived.astype(jnp.float32)
    normed_one = norm_rows(inputs, gain_one, shift_one)
    normed_low = normed_one.astype(jnp.bfloat16)
    joint = forward_dot(normed_low, project_full)
    queries = (joint[:, :width] + query_full).astype(jnp.bfloat16).reshape(total_rows, HEADS, HEAD)
    key_rows = joint[:, width : 2 * width].astype(jnp.bfloat16).reshape(total_rows, HEADS, HEAD)
    value_rows = (joint[:, 2 * width :] + value_full).astype(jnp.bfloat16).reshape(total_rows, HEADS, HEAD)
    score_scale = HEAD ** (-0.5)
    visible = labels[:, None] == labels[None, :]

    def block_scores():
        raw_scores = matmul(queries, key_rows, "qhe,khe->hqk") * score_scale
        return jnp.where(visible[None], raw_scores, MASK_VALUE)

    scores = block_scores()
    top_score = jnp.max(scores, axis=-1, keepdims=True)
    weights = jnp.exp(scores - top_score)
    totals = jnp.sum(weights, axis=-1, keepdims=True)
    prob_low = (weights / totals).astype(jnp.bfloat16)
    mixed_rows = matmul(prob_low, value_rows, "hqk,khe->qhe")
    log_totals = top_score + jnp.log(totals)
    attended = mixed_rows.astype(jnp.bfloat16).reshape(total_rows, width)
    attn_out = forward_dot(attended, output_full) + outbias_full
    hidden = inputs + attn_out
    normed_two = norm_rows(hidden, gain_two, shift_two)
    normed_two_low = normed_two.astype(jnp.bfloat16)
    pre_act = forward_dot(normed_two_low, up_full) + upbias_full
    activated = gelu_exact(pre_act).astype(jnp.bfloat16)
    branch = forward_dot(activated, down_full) + downbias_full
    encoded_rows = live_rows * (hidden + branch)
    encoded_back = lax.all_to_all(
        encoded_rows.astype(jnp.bfloat16), dp_names, split_axis=0, concat_axis=0, tiled=True
    )

    grad_out = live_rows * cot_rows.astype(jnp.float32)
    grad_branch = grad_out.astype(jnp.bfloat16)
    down_low = weight_grad(activated, grad_branch)
    grad_downbias = column_sums(grad_branch)
    grad_activ = backward_dot(grad_branch, down_full)
    grad_pre = jax.vjp(gelu_exact, pre_act)[1](grad_activ)[0].astype(jnp.bfloat16)
    up_low = weight_grad(normed_two_low, grad_pre)
    grad_upbias = column_sums(grad_pre)
    grad_normed_two = backward_dot(grad_pre, up_full)
    norm_pull_two = jax.vjp(norm_rows, hidden, gain_two, shift_two)[1]
    grad_hidden_part, grad_gain_two, grad_shift_two = norm_pull_two(grad_normed_two)
    grad_hidden = grad_out + grad_hidden_part
    grad_hidden, down_low, up_low = lax.optimization_barrier((grad_hidden, down_low, up_low))
    down_part = scatter_matrix(down_low, down_weight.shape[0])
    up_part = scatter_matrix(up_low, up_weight.shape[0])

    grad_attn = grad_hidden.astype(jnp.bfloat16)
    output_low = weight_grad(attended, grad_attn)
    grad_outbias = column_sums(grad_attn)
    grad_attended = backward_dot(grad_attn, output_full).astype(jnp.bfloat16).reshape(total_rows, HEADS, HEAD)
    grad_attended, output_low = lax.optimization_barrier((grad_attended, output_low))

    scores = block_scores()
    prob_full = jnp.exp(scores - log_totals)
    prob_low = prob_full.astype(jnp.bfloat16)
    value_grad = matmul(prob_low, grad_attended, "hqk,qhe->khe")
    grad_prob = matmul(grad_attended, value_rows, "qhe,khe->hqk")
    inner = jnp.sum(prob_full * grad_prob, axis=-1, keepdims=True)
    grad_scores = (prob_full * (grad_prob - inner)).astype(jnp.bfloat16)
    query_grad = matmul(grad_scores, key_rows, "hqk,khe->qhe") * score_scale
    key_grad = matmul(grad_scores, queries, "hqk,qhe->khe") * score_scale
    grad_queries = query_grad.astype(jnp.bfloat16).reshape(total_rows, width)
    grad_keys = key_grad.reshape(total_rows, width).astype(jnp.bfloat16)
    grad_values = value_grad.reshape(total_rows, width).astype(jnp.bfloat16)
    grad_joint = jnp.concatenate([grad_queries, grad_keys, grad_values], axis=1)
    project_low = weight_grad(normed_low, grad_joint)
    grad_querybias = column_sums(grad_queries)
    grad_valuebias = column_sums(grad_values)
    out_cols = output_low.shape[-1]
    joined_low = jnp.concatenate(
        [output_low.reshape(*weights_tree.sizes, output_weight.shape[0], out_cols),
         project_low.reshape(*weights_tree.sizes, project_weight.shape[0], project_low.shape[-1])], axis=-1)
    joined_part = weights_tree.scatter(joined_low, jnp.bfloat16)
    output_part = joined_part[:, :out_cols]
    project_part = joined_part[:, out_cols:]
    grad_normed_one = backward_dot(grad_joint, project_full)
    norm_pull_one = jax.vjp(norm_rows, inputs, gain_one, shift_one)[1]
    grad_input_part, grad_gain_one, grad_shift_one = norm_pull_one(grad_normed_one)
    grad_inputs = grad_hidden + grad_input_part
    grad_back = lax.all_to_all(
        grad_inputs.astype(jnp.bfloat16), dp_names, split_axis=0, concat_axis=0, tiled=True
    )

    vector_grads = (
        grad_gain_one, grad_shift_one, grad_querybias, grad_valuebias, grad_outbias,
        grad_gain_two, grad_shift_two, grad_upbias, grad_downbias,
    )
    stacked = jnp.concatenate([g.reshape(n_dp, -1) for g in vector_grads], axis=1)
    stacked = stacked + lax.ppermute(stacked, "fsdp", [(i, (i + 1) % n_fsdp) for i in range(n_fsdp)])
    mine = vectors_tree.scatter(stacked.reshape(*vectors_tree.sizes, -1), jnp.float32)
    sums = []
    offset = 0
    for w in widths:
        sums.append(mine[offset : offset + w])
        offset += w
    (g_gain_one, g_shift_one, g_querybias, g_valuebias, g_outbias,
     g_gain_two, g_shift_two, g_upbias, g_downbias) = sums

    return (
        encoded_back, grad_back, g_gain_one, g_shift_one, project_part, g_querybias, g_valuebias,
        output_part, g_outbias, g_gain_two, g_shift_two, up_part, g_upbias, down_part, g_downbias,
    )


def solution(mesh):
    n_dp, n_fsdp = mesh.shape["dp"], mesh.shape["fsdp"]
    phys, dp_names, weights_tree, vectors_tree = build(mesh)
    rows = P((*dp_names, "fsdp"), None)
    matrix = P(dp_names, "fsdp")
    vector = P(dp_names)

    def step(*args):
        return local(dp_names, weights_tree, vectors_tree, n_dp, n_fsdp, *args)

    return jax.shard_map(
        step,
        mesh=phys,
        in_specs=(rows, rows, rows, P((*dp_names, "fsdp")), vector, vector, matrix, vector, vector,
                  matrix, vector, vector, vector, matrix, vector, matrix, vector),
        out_specs=(rows, rows, vector, vector, matrix, vector, vector, matrix, vector, vector,
                   vector, matrix, vector, matrix, vector),
        check_vma=False,
    )
```
